32 devices in a mesh: slab: 2 (over y), date: 8 (over z, x), tile: 1, sub: 2 (over core).
Axes of the slice: x: 2, y: 2, z: 4, core: 2. Of those that a mesh axis runs over, the one named last changes fastest.
Arguments:
- slc: bfloat16 [2, 100, 128, 512], P(None, None, 'date', ('slab', 'tile', 'sub')), parts along dimension 3, may hold values from -300 to 300, as said below
- usable: int32 [100, 128, 512], P(None, 'date', ('slab', 'tile', 'sub')), parts along dimension 2, may hold values 0 or 1
Outputs:
- coherence: bfloat16 [2, 4, 8, 16, 128, 128], P(None, ('slab', 'tile', 'sub'), 'date'), parts along dimension 1
- linked: float32 [2, 128, 512], P(None, 'date', ('slab', 'tile', 'sub')), parts along dimension 2
The draws below stay inside these ranges and needn't reach their ends.
There are 2 independent parts, one for each index of `slab`. The reference program is written for one: setup_inputs(seed, part) draws one part's arguments, and reference() takes and returns one part's arrays. A program takes and returns all parts, laid end to end along the dimension named above; each array names one. Nothing has to cross between parts.
Inputs may be any that keep to these rules, and one draw needn't show every extreme that they name: `slc`: complex samples of a partly coherent stack.
All inputs are finite; a program needn't handle non-finite values. No bound on the sum of `usable` on one device may be relied on, other than what follows from the above.
Results may differ from the reference program's by a relative error of at most 0.0016.
Values may be sent and summed in bfloat16 or wider, within the bound.
No kernel may reach another device: no remote copies, remote signals or barrier semaphores. Data moves between devices by JAX's collectives and lax.ppermute only.
A program may use at most 64 MiB of HBM per device.

```python
import math
import jax
import jax.numpy as jnp
from jax import lax

DATES = 128
LOOKS = 100
ITERS = 4
WD = 16
WT = 128
NG = 2
NB = 8
WIN = 256


def rotate(common, phase):
    cosine = jnp.cos(phase)[None]
    sine_part = jnp.sin(phase)[None]
    return jnp.stack([common[0] * cosine - common[1] * sine_part, common[0] * sine_part + common[1] * cosine])


def draw_slc(key, part):
    subkeys = jax.random.split(key, 9)
    grid_shape = (DATES, WIN)
    amplitude = jnp.exp(jax.random.uniform(subkeys[0], grid_shape, jnp.float32, 0.0, math.log(10.0)))
    speckle = jnp.clip(jax.random.normal(subkeys[8], (2, LOOKS, DATES, WIN), jnp.float32), -4.0, 4.0)
    first_phase = jax.random.uniform(subkeys[1], grid_shape, jnp.float32, -math.pi, math.pi)
    second_phase = jax.random.uniform(subkeys[2], grid_shape, jnp.float32, -math.pi, math.pi)
    first_weight = jax.random.uniform(subkeys[3], (WIN,), jnp.float32, 0.3, 0.9)
    second_weight = jax.random.uniform(subkeys[4], (WIN,), jnp.float32, 0.1, 0.4)
    first_common = jnp.clip(jax.random.normal(subkeys[5], (2, LOOKS, 1, WIN), jnp.float32), -4.0, 4.0)
    second_common = jnp.clip(jax.random.normal(subkeys[6], (2, LOOKS, 1, WIN), jnp.float32), -4.0, 4.0)
    noise_weight = jnp.sqrt(jnp.maximum(1.0 - first_weight * first_weight - second_weight * second_weight, 0.05))
    sample = first_weight * rotate(first_common, first_phase) + second_weight * rotate(second_common, second_phase) + noise_weight * speckle
    return (amplitude * sample).astype(jnp.bfloat16)


def set_ends(drawn, stream_key, low, high):
    dims = drawn.shape
    place = [jax.random.randint(jax.random.fold_in(stream_key, axis), (), 0, dims[axis]) for axis in range(len(dims))]
    drawn = drawn.at[tuple(place)].set(low)
    longest = dims.index(max(dims))
    place[longest] = (place[longest] + 1) % dims[longest]
    return drawn.at[tuple(place)].set(high)


def setup_inputs(seed: int = 0, part: int = 0) -> dict:
    seeds = jax.random.split(jax.random.key(seed), 3)
    own_keys = jax.random.split(jax.random.fold_in(seeds[2], part), 3)
    return {
        "slc": draw_slc(jax.random.fold_in(jax.random.fold_in(seeds[2], part), 71), part),
        "usable": set_ends((jax.random.randint(own_keys[1], (LOOKS, DATES, WIN), 0, 4) < 3).astype(jnp.int32), jax.random.fold_in(own_keys[1], 1), 0, 1),
    }


def link_vectors(coherence):
    matrix = coherence.astype(jnp.float32)
    vec_real = jnp.ones((DATES, matrix.shape[1]), jnp.float32)
    vec_imag = jnp.zeros((DATES, matrix.shape[1]), jnp.float32)
    for step in range(ITERS):
        rr = jnp.einsum('wab,bw->aw', matrix[0], vec_real, precision=lax.Precision.HIGHEST)
        ii = jnp.einsum('wab,bw->aw', matrix[1], vec_imag, precision=lax.Precision.HIGHEST)
        ri = jnp.einsum('wab,bw->aw', matrix[0], vec_imag, precision=lax.Precision.HIGHEST)
        ir = jnp.einsum('wab,bw->aw', matrix[1], vec_real, precision=lax.Precision.HIGHEST)
        new_real = rr - ii
        new_imag = ri + ir
        scale = lax.rsqrt(lax.optimization_barrier(jnp.mean(new_real * new_real + new_imag * new_imag, axis=0)) + 1e-05)
        vec_real = new_real * scale[None]
        vec_imag = new_imag * scale[None]
    return jnp.stack([vec_real, vec_imag])

def window_block(operands):
    block, root = operands
    real_sum = jnp.einsum('law,lbw->wab', block[0], block[0]) + jnp.einsum('law,lbw->wab', block[1], block[1])
    imag_sum = jnp.einsum('law,lbw->wab', block[1], block[0]) - jnp.einsum('law,lbw->wab', block[0], block[1])
    factor = root.T[:, :, None] * root.T[:, None, :] * (1.0 / LOOKS)
    coherence = jnp.stack([real_sum * factor, imag_sum * factor]).astype(jnp.bfloat16)
    return (coherence, link_vectors(coherence))

def reference(slc, usable):
    masked = slc * usable.astype(jnp.bfloat16)[None]
    samples = masked.astype(jnp.float32)
    intensity = lax.optimization_barrier(jnp.mean(samples[0] * samples[0] + samples[1] * samples[1], axis=0)) + 1e-05
    inverse_root = lax.rsqrt(intensity)
    blocks = jnp.moveaxis(samples.reshape(2, LOOKS, DATES, NG, WT), 3, 0)
    roots = jnp.moveaxis(inverse_root.reshape(DATES, NG, WT), 1, 0)
    coherence, linked = lax.map(window_block, (blocks, roots))
    coherence = jnp.moveaxis(coherence, 1, 0)
    linked = jnp.moveaxis(linked, 0, 2).reshape(2, DATES, WIN)
    return (coherence.reshape(2, NG, NB, WD, DATES, DATES), linked)
```

```python
import jax
import jax.numpy as jnp
from jax import lax
from jax.experimental import pallas as pl
from jax.experimental.pallas import tpu as pltpu
from jax.sharding import PartitionSpec as P

ITERS = 4
EPS = 1e-05
SUB = 8


def pack_blocks(slc, usable, position, blocks):
    parts, looks, dates, windows = slc.shape
    per_device = windows // blocks
    chunk = blocks // parts
    groups = looks // chunk
    per_step = max(n for n in range(1, 6) if groups % n == 0)

    def kernel(shift_ref, slc_ref, usable_ref, *out_refs):
        shift = shift_ref[0]
        lane = lax.broadcasted_iota(jnp.int32, (dates, windows), 1)
        for step in range(per_step):
            rows = []
            flags = [usable_ref[step * chunk + look].astype(jnp.float32) for look in range(chunk)]
            for part in range(parts):
                for look in range(chunk):
                    sample = slc_ref[part, step * chunk + look].astype(jnp.float32)
                    rows.append(pltpu.roll(sample * flags[look], shift, 1))
            stride = blocks // 2
            while stride:
                width = stride * per_device
                low_half = (lane & width) == 0
                for index in range(blocks):
                    if index & stride:
                        continue
                    low, high = rows[index], rows[index + stride]
                    rows[index] = jnp.where(low_half, low, pltpu.roll(high, width, 1))
                    rows[index + stride] = jnp.where(
                        low_half, pltpu.roll(low, windows - width, 1), high
                    )
                stride //= 2
            for index in range(blocks):
                out_refs[index][step] = rows[index].astype(jnp.bfloat16)

    piece = jax.ShapeDtypeStruct((groups, dates, windows), jnp.bfloat16)
    shift = (windows - per_device * position) % windows
    return pl.pallas_call(
        kernel,
        grid=(groups // per_step,),
        in_specs=[
            pl.BlockSpec(memory_space=pltpu.SMEM),
            pl.BlockSpec((parts, per_step * chunk, dates, windows), lambda n: (0, n, 0, 0)),
            pl.BlockSpec((per_step * chunk, dates, windows), lambda n: (n, 0, 0)),
        ],
        out_specs=[pl.BlockSpec((per_step, dates, windows), lambda n: (n, 0, 0))] * blocks,
        out_shape=[piece] * blocks,
        name="pack_blocks",
    )(shift.astype(jnp.int32).reshape(1), slc, usable)


def link_windows(pieces, position, looks_count, per_device):
    blocks = len(pieces)
    groups, dates, width = pieces[0].shape
    total = blocks * dates
    rows_count = groups * blocks
    half = blocks // 2
    date_tiles = dates // SUB
    per_step = 2

    def kernel(position_ref, *refs):
        piece_refs = refs[:blocks]
        coherence_ref, packed_ref, stacked, samples = refs[blocks:]
        step = pl.program_id(0)

        @pl.when(step == 0)
        def _():
            for index in range(blocks):
                source = lax.rem(position_ref[0] + (blocks - index), blocks)
                start = pl.multiple_of(source * dates, dates)
                stacked[:, pl.ds(start, dates), :] = piece_refs[index][...]
            row = lax.broadcasted_iota(jnp.int32, (width, width), 0)
            col = lax.broadcasted_iota(jnp.int32, (width, width), 1)
            wanted = lax.rem(row, blocks) * per_device + lax.div(row, blocks)
            select = jnp.where(wanted == col, 1.0, 0.0).astype(jnp.bfloat16)
            for group in range(groups):
                turned = lax.dot_general(
                    select, stacked[group], (((1,), (1,)), ((), ())),
                    preferred_element_type=jnp.float32,
                )
                samples[:, group * blocks : (group + 1) * blocks, :] = turned.reshape(
                    per_device, blocks, total
                )
            packed_ref[...] = jnp.zeros_like(packed_ref)

        lane = lax.broadcasted_iota(jnp.int32, (SUB, width), 1)
        diagonal = lax.broadcasted_iota(jnp.int32, (total, total), 0) == lax.broadcasted_iota(
            jnp.int32, (total, total), 1
        )
        part_sign = jnp.where(
            lax.broadcasted_iota(jnp.int32, (groups, blocks, total), 1) < half, -1.0, 1.0
        )
        for index in range(per_step):
            window = step * per_step + index
            left = samples[window]
            turned = pltpu.roll(left.reshape(groups, blocks, total), half, 1) * part_sign
            left = left.astype(jnp.bfloat16)
            right = jnp.concatenate(
                [left, turned.reshape(rows_count, total).astype(jnp.bfloat16)], axis=1
            )
            cross = lax.dot_general(
                left, right, (((0,), (0,)), ((), ())), preferred_element_type=jnp.float32
            )
            cross_real = cross[:, :total]
            cross_imag = cross[:, total:]
            power = jnp.where(diagonal, cross_real, 0.0)
            root_row = lax.rsqrt(jnp.sum(power, axis=0, keepdims=True) / looks_count + EPS)
            root_col = lax.rsqrt(jnp.sum(power, axis=1, keepdims=True) / looks_count + EPS)
            factor = root_col * root_row * (1.0 / looks_count)
            real = (cross_real * factor).astype(jnp.bfloat16)
            imag = (cross_imag * factor).astype(jnp.bfloat16)
            coherence_ref[0, index] = real
            coherence_ref[1, index] = imag
            real = real.astype(jnp.float32)
            imag = imag.astype(jnp.float32)
            z0 = jnp.sum(real, axis=0, keepdims=True)
            z1 = -jnp.sum(imag, axis=0, keepdims=True)
            for iteration in range(ITERS):
                axis = 1 if iteration % 2 == 0 else 0
                scale = lax.rsqrt(
                    jnp.sum(z0 * z0 + z1 * z1, axis=axis, keepdims=True) / total + EPS
                )
                v0 = z0 * scale
                v1 = z1 * scale
                if iteration == ITERS - 1:
                    break
                if axis == 1:
                    z0 = jnp.sum(real * v0 - imag * v1, axis=1, keepdims=True)
                    z1 = jnp.sum(real * v1 + imag * v0, axis=1, keepdims=True)
                else:
                    z0 = jnp.sum(real * v0 + imag * v1, axis=0, keepdims=True)
                    z1 = jnp.sum(real * v1 - imag * v0, axis=0, keepdims=True)
            for block in range(blocks):
                kept = packed_ref[block]
                for part, vector in enumerate((v0, v1)):
                    for tile in range(date_tiles):
                        start = block * dates + tile * SUB
                        slot = (part * date_tiles + tile) * per_device + window
                        kept = jnp.where(lane == slot, vector[start : start + SUB], kept)
                packed_ref[block] = kept

    whole = pl.BlockSpec((groups, dates, width), lambda n: (0, 0, 0))
    return pl.pallas_call(
        kernel,
        grid=(per_device // per_step,),
        in_specs=[pl.BlockSpec(memory_space=pltpu.SMEM)] + [whole] * blocks,
        out_specs=[
            pl.BlockSpec((2, per_step, total, total), lambda n: (0, n, 0, 0)),
            pl.BlockSpec((blocks, SUB, width), lambda n: (0, 0, 0)),
        ],
        out_shape=[
            jax.ShapeDtypeStruct((2, per_device, total, total), jnp.bfloat16),
            jax.ShapeDtypeStruct((blocks, SUB, width), jnp.float32),
        ],
        scratch_shapes=[
            pltpu.VMEM((groups, total, width), jnp.bfloat16),
            pltpu.VMEM((per_device, rows_count, total), jnp.float32),
        ],
        name="link_windows",
    )(position.astype(jnp.int32).reshape(1), *pieces)


def unpack_linked(packed, dates, per_device):
    blocks, _, width = packed.shape
    date_tiles = dates // SUB

    def kernel(packed_ref, out_ref):
        lane = lax.broadcasted_iota(jnp.int32, (SUB, width), 1)
        owner = lax.div(lane, per_device)
        for part in range(2):
            for tile in range(date_tiles):
                held = (part * date_tiles + tile) * per_device
                row = jnp.zeros((SUB, width), jnp.float32)
                for source in range(blocks):
                    shift = (source * per_device - held) % width
                    moved = packed_ref[source]
                    if shift:
                        moved = pltpu.roll(moved, shift, 1)
                    row = jnp.where(owner == source, moved, row)
                out_ref[part, tile * SUB : (tile + 1) * SUB, :] = row

    return pl.pallas_call(
        kernel,
        out_shape=jax.ShapeDtypeStruct((2, dates, width), jnp.float32),
        name="unpack_linked",
    )(packed)


def local(slc, usable):
    looks_count = slc.shape[1]
    own_dates = slc.shape[2]
    windows = slc.shape[3]
    blocks = lax.axis_size("date")
    per_device = windows // blocks
    position = lax.axis_index("date")
    chunk = blocks // 2
    extra = -looks_count % chunk
    if extra:
        slc = jnp.pad(slc, ((0, 0), (0, extra), (0, 0), (0, 0)))
        usable = jnp.pad(usable, ((0, extra), (0, 0), (0, 0)))
    pieces = pack_blocks(slc, usable, position, blocks)
    order = sorted(range(1, blocks), key=lambda hop: abs(hop - blocks // 2))
    received = [pieces[0]] + [None] * (blocks - 1)
    for hop in order:
        pairs = [(source, (source + hop) % blocks) for source in range(blocks)]
        received[hop] = lax.ppermute(pieces[hop], "date", pairs)
    coherence, packed = link_windows(received, position, looks_count, per_device)
    packed = lax.all_to_all(packed, "date", split_axis=0, concat_axis=0, tiled=True)
    linked = unpack_linked(packed, own_dates, per_device)
    total = own_dates * blocks
    return (coherence.reshape(2, 1, 1, per_device, total, total), linked)


def solution(mesh):
    return jax.shard_map(
        local,
        mesh=mesh,
        in_specs=(
            P(None, None, "date", ("slab", "tile", "sub")),
            P(None, "date", ("slab", "tile", "sub")),
        ),
        out_specs=(
            P(None, ("slab", "tile", "sub"), "date", None, None, None),
            P(None, "date", ("slab", "tile", "sub")),
        ),
        check_vma=False,
    )
```

```python
import jax
import jax.numpy as jnp
from jax import lax
from jax.experimental import pallas as pl
from jax.experimental.pallas import tpu as pltpu
from jax.sharding import PartitionSpec as P

ITERS = 4
EPS = 1e-05
SUB = 8


def on_chip(array):
    return pltpu.with_memory_space_constraint(array, pltpu.VMEM)


def pack_blocks(slc, usable, position, blocks):
    parts, looks, dates, windows = slc.shape
    per_device = windows // blocks
    chunk = blocks // parts
    groups = looks // chunk
    per_step = max(n for n in range(1, 6) if groups % n == 0)

    def kernel(shift_ref, slc_ref, usable_ref, *out_refs):
        shift = shift_ref[0]
        lane = lax.broadcasted_iota(jnp.int32, (dates, windows), 1)
        for step in range(per_step):
            rows = []
            flags = [usable_ref[step * chunk + look].astype(jnp.float32) for look in range(chunk)]
            for part in range(parts):
                for look in range(chunk):
                    sample = slc_ref[part, step * chunk + look].astype(jnp.float32)
                    rows.append(pltpu.roll(sample * flags[look], shift, 1))
            stride = blocks // 2
            while stride:
                width = stride * per_device
                low_half = (lane & width) == 0
                for index in range(blocks):
                    if index & stride:
                        continue
                    low, high = rows[index], rows[index + stride]
                    rows[index] = jnp.where(low_half, low, pltpu.roll(high, width, 1))
                    rows[index + stride] = jnp.where(
                        low_half, pltpu.roll(low, windows - width, 1), high
                    )
                stride //= 2
            for index in range(blocks):
                out_refs[index][step] = rows[index].astype(jnp.bfloat16)

    piece = pltpu.VMEM((groups, dates, windows), jnp.bfloat16)
    shift = (windows - per_device * position) % windows
    return pl.pallas_call(
        kernel,
        grid=(groups // per_step,),
        in_specs=[
            pl.BlockSpec(memory_space=pltpu.SMEM),
            pl.BlockSpec((parts, per_step * chunk, dates, windows), lambda n: (0, n, 0, 0)),
            pl.BlockSpec((per_step * chunk, dates, windows), lambda n: (n, 0, 0)),
        ],
        out_specs=[pl.BlockSpec((per_step, dates, windows), lambda n: (n, 0, 0))] * blocks,
        out_shape=[piece] * blocks,
        name="pack_blocks",
    )(shift.astype(jnp.int32).reshape(1), slc, usable)


def link_windows(pieces, position, looks_count, per_device):
    blocks = len(pieces)
    groups, dates, width = pieces[0].shape
    total = blocks * dates
    rows_count = groups * blocks
    half = blocks // 2
    date_tiles = dates // SUB
    per_step = 4

    def kernel(position_ref, *refs):
        piece_refs = refs[:blocks]
        coherence_ref, packed_ref, stacked, samples = refs[blocks:]
        step = pl.program_id(0)

        @pl.when(step == 0)
        def _():
            for index in range(blocks):
                source = lax.rem(position_ref[0] + (blocks - index), blocks)
                start = pl.multiple_of(source * dates, dates)
                stacked[:, pl.ds(start, dates), :] = piece_refs[index][...]
            row = lax.broadcasted_iota(jnp.int32, (width, width), 0)
            col = lax.broadcasted_iota(jnp.int32, (width, width), 1)
            wanted = lax.rem(row, blocks) * per_device + lax.div(row, blocks)
            select = jnp.where(wanted == col, 1.0, 0.0).astype(jnp.bfloat16)
            for group in range(groups):
                turned = lax.dot_general(
                    select, stacked[group], (((1,), (1,)), ((), ())),
                    preferred_element_type=jnp.float32,
                )
                samples[:, group * blocks : (group + 1) * blocks, :] = turned.reshape(
                    per_device, blocks, total
                )
            packed_ref[...] = jnp.zeros_like(packed_ref)

        lane = lax.broadcasted_iota(jnp.int32, (SUB, width), 1)
        diagonal = lax.broadcasted_iota(jnp.int32, (total, total), 0) == lax.broadcasted_iota(
            jnp.int32, (total, total), 1
        )
        part_sign = jnp.where(
            lax.broadcasted_iota(jnp.int32, (groups, blocks, total), 1) < half, -1.0, 1.0
        )
        for index in range(per_step):
            window = step * per_step + index
            left = samples[window]
            turned = pltpu.roll(left.reshape(groups, blocks, total), half, 1) * part_sign
            left = left.astype(jnp.bfloat16)
            right = jnp.concatenate(
                [left, turned.reshape(rows_count, total).astype(jnp.bfloat16)], axis=1
            )
            cross = lax.dot_general(
                left, right, (((0,), (0,)), ((), ())), preferred_element_type=jnp.float32
            )
            cross_real = cross[:, :total]
            cross_imag = cross[:, total:]
            power = jnp.where(diagonal, cross_real, 0.0)
            root_row = lax.rsqrt(jnp.sum(power, axis=0, keepdims=True) / looks_count + EPS)
            root_col = lax.rsqrt(jnp.sum(power, axis=1, keepdims=True) / looks_count + EPS)
            factor = root_col * root_row * (1.0 / looks_count)
            real = (cross_real * factor).astype(jnp.bfloat16)
            imag = (cross_imag * factor).astype(jnp.bfloat16)
            coherence_ref[0, index] = real
            coherence_ref[1, index] = imag
            real = real.astype(jnp.float32)
            imag = imag.astype(jnp.float32)
            z0 = jnp.sum(real, axis=0, keepdims=True)
            z1 = -jnp.sum(imag, axis=0, keepdims=True)
            for iteration in range(ITERS):
                axis = 1 if iteration % 2 == 0 else 0
                scale = lax.rsqrt(
                    jnp.sum(z0 * z0 + z1 * z1, axis=axis, keepdims=True) / total + EPS
                )
                v0 = z0 * scale
                v1 = z1 * scale
                if iteration == ITERS - 1:
                    break
                if axis == 1:
                    z0 = jnp.sum(real * v0 - imag * v1, axis=1, keepdims=True)
                    z1 = jnp.sum(real * v1 + imag * v0, axis=1, keepdims=True)
                else:
                    z0 = jnp.sum(real * v0 + imag * v1, axis=0, keepdims=True)
                    z1 = jnp.sum(real * v1 - imag * v0, axis=0, keepdims=True)
            for block in range(blocks):
                kept = packed_ref[block]
                for part, vector in enumerate((v0, v1)):
                    for tile in range(date_tiles):
                        start = block * dates + tile * SUB
                        slot = (part * date_tiles + tile) * per_device + window
                        kept = jnp.where(lane == slot, vector[start : start + SUB], kept)
                packed_ref[block] = kept

    whole = pl.BlockSpec(memory_space=pltpu.VMEM)
    return pl.pallas_call(
        kernel,
        grid=(per_device // per_step,),
        in_specs=[pl.BlockSpec(memory_space=pltpu.SMEM)] + [whole] * blocks,
        out_specs=[
            pl.BlockSpec((2, per_step, total, total), lambda n: (0, n, 0, 0)),
            pl.BlockSpec(memory_space=pltpu.VMEM),
        ],
        out_shape=[
            pltpu.VMEM((2, per_device, total, total), jnp.bfloat16),
            pltpu.VMEM((blocks, SUB, width), jnp.float32),
        ],
        scratch_shapes=[
            pltpu.VMEM((groups, total, width), jnp.bfloat16),
            pltpu.VMEM((per_device, rows_count, total), jnp.float32),
        ],
        name="link_windows",
    )(position.astype(jnp.int32).reshape(1), *[on_chip(piece) for piece in pieces])


def unpack_linked(packed, dates, per_device):
    blocks, _, width = packed.shape
    date_tiles = dates // SUB

    def kernel(packed_ref, out_ref):
        lane = lax.broadcasted_iota(jnp.int32, (SUB, width), 1)
        owner = lax.div(lane, per_device)
        for part in range(2):
            for tile in range(date_tiles):
                held = (part * date_tiles + tile) * per_device
                row = jnp.zeros((SUB, width), jnp.float32)
                for source in range(blocks):
                    shift = (source * per_device - held) % width
                    moved = packed_ref[source]
                    if shift:
                        moved = pltpu.roll(moved, shift, 1)
                    row = jnp.where(owner == source, moved, row)
                out_ref[part, tile * SUB : (tile + 1) * SUB, :] = row

    return pl.pallas_call(
        kernel,
        in_specs=[pl.BlockSpec(memory_space=pltpu.VMEM)],
        out_specs=pl.BlockSpec(memory_space=pltpu.VMEM),
        out_shape=jax.ShapeDtypeStruct((2, dates, width), jnp.float32),
        name="unpack_linked",
    )(on_chip(packed))


def local(slc, usable):
    looks_count = slc.shape[1]
    own_dates = slc.shape[2]
    windows = slc.shape[3]
    blocks = lax.axis_size("date")
    per_device = windows // blocks
    position = lax.axis_index("date")
    chunk = blocks // 2
    extra = -looks_count % chunk
    if extra:
        slc = jnp.pad(slc, ((0, 0), (0, extra), (0, 0), (0, 0)))
        usable = jnp.pad(usable, ((0, extra), (0, 0), (0, 0)))
    pieces = pack_blocks(slc, usable, position, blocks)
    order = sorted(range(1, blocks), key=lambda hop: abs(hop - blocks // 2))
    received = [pieces[0]] + [None] * (blocks - 1)
    for hop in order:
        pairs = [(source, (source + hop) % blocks) for source in range(blocks)]
        received[hop] = lax.ppermute(pieces[hop], "date", pairs)
    coherence, packed = link_windows(received, position, looks_count, per_device)
    packed = lax.all_to_all(packed, "date", split_axis=0, concat_axis=0, tiled=True)
    linked = unpack_linked(packed, own_dates, per_device)
    total = own_dates * blocks
    return (coherence.reshape(2, 1, 1, per_device, total, total), linked)


def solution(mesh):
    return jax.shard_map(
        local,
        mesh=mesh,
        in_specs=(
            P(None, None, "date", ("slab", "tile", "sub")),
            P(None, "date", ("slab", "tile", "sub")),
        ),
        out_specs=(
            P(None, ("slab", "tile", "sub"), "date", None, None, None),
            P(None, "date", ("slab", "tile", "sub")),
        ),
        check_vma=False,
    )
```

```python
import jax
import jax.numpy as jnp
from jax import lax
from jax.experimental import pallas as pl
from jax.experimental.pallas import tpu as pltpu
from jax.sharding import PartitionSpec as P

ITERS = 4
EPS = 1e-05
SUB = 8


def on_chip(array):
    return pltpu.with_memory_space_constraint(array, pltpu.VMEM)


def pack_blocks(slc, usable, position, order):
    blocks = len(order)
    parts, looks, dates, windows = slc.shape
    per_device = windows // blocks
    chunk = blocks // parts
    groups = looks // chunk
    per_step = max(n for n in range(1, 6) if groups % n == 0)

    def kernel(shift_ref, slc_ref, usable_ref, *out_refs):
        shift = shift_ref[0]
        lane = lax.broadcasted_iota(jnp.int32, (dates, windows), 1).astype(jnp.int16)
        for step in range(per_step):
            rows = []
            flags = [usable_ref[step * chunk + look].astype(jnp.bfloat16) for look in range(chunk)]
            for part in range(parts):
                for look in range(chunk):
                    sample = slc_ref[part, step * chunk + look]
                    rows.append(pltpu.roll(sample * flags[look], shift, 1))
            stride = blocks // 2
            while stride:
                width = stride * per_device
                low_half = (lane & width) == 0
                for index in range(blocks):
                    if index & stride:
                        continue
                    low, high = rows[index], rows[index + stride]
                    rows[index] = jnp.where(low_half, low, pltpu.roll(high, width, 1))
                    rows[index + stride] = jnp.where(
                        low_half, pltpu.roll(low, windows - width, 1), high
                    )
                stride //= 2
            for index, hop in enumerate(order):
                out_refs[index][pl.program_id(0) * per_step + step] = rows[hop]

    piece = pltpu.VMEM((groups, dates, windows), jnp.bfloat16)
    shift = (windows - per_device * position) % windows
    return pl.pallas_call(
        kernel,
        grid=(groups // per_step,),
        in_specs=[
            pl.BlockSpec(memory_space=pltpu.SMEM),
            pl.BlockSpec((parts, per_step * chunk, dates, windows), lambda n: (0, n, 0, 0)),
            pl.BlockSpec((per_step * chunk, dates, windows), lambda n: (n, 0, 0)),
        ],
        out_specs=[pl.BlockSpec(memory_space=pltpu.VMEM)] * blocks,
        out_shape=[piece] * blocks,
        name="pack_blocks",
    )(shift.astype(jnp.int32).reshape(1), slc, usable)


def link_windows(pieces, order, position, looks_count, per_device):
    blocks = len(pieces)
    groups, dates, width = pieces[0].shape
    total = blocks * dates
    pairs = (groups + 1) // 2
    half = blocks // 2
    date_tiles = dates // SUB
    per_step = 4

    def kernel(position_ref, *refs):
        piece_refs = refs[:blocks]
        coherence_ref, packed_ref, stacked, samples, vectors = refs[blocks:]
        step = pl.program_id(0)

        @pl.when(step == 0)
        def _():
            for index, hop in enumerate(order):
                source = lax.rem(position_ref[0] + (blocks - hop), blocks)
                start = pl.multiple_of(source * dates, dates)
                stacked[:, pl.ds(start, dates), :] = piece_refs[index][...]
            row = lax.broadcasted_iota(jnp.int32, (2 * width, 2 * width), 0)
            col = lax.broadcasted_iota(jnp.int32, (2 * width, 2 * width), 1)
            inner = lax.rem(col, width)
            slot = lax.div(inner, per_device)
            wanted = (
                lax.rem(inner, per_device) * (2 * blocks)
                + lax.div(slot, half) * blocks
                + lax.div(col, width) * half
                + lax.rem(slot, half)
            )
            select = jnp.where(wanted == row, 1.0, 0.0).astype(jnp.bfloat16)
            for pair in range(pairs):
                first = 2 * pair
                if first + 1 < groups:
                    block = jnp.concatenate([stacked[first], stacked[first + 1]], axis=1)
                    chosen = select
                else:
                    block = stacked[first]
                    chosen = select[:, :width]
                turned = lax.dot_general(
                    chosen, block, (((1,), (1,)), ((), ())), preferred_element_type=jnp.float32
                )
                samples[:, :, pair * blocks : (pair + 1) * blocks, :] = turned.reshape(
                    per_device, 2, blocks, total
                )
            vectors[...] = jnp.zeros_like(vectors)

        ones = jnp.ones((total, total), jnp.bfloat16)
        diagonal = lax.broadcasted_iota(jnp.int32, (total, total), 0) == lax.broadcasted_iota(
            jnp.int32, (total, total), 1
        )
        for index in range(per_step):
            window = step * per_step + index
            real_part = samples[window, 0]
            imag_part = samples[window, 1]
            left = jnp.concatenate([real_part, imag_part], axis=0).astype(jnp.bfloat16)
            turned = jnp.concatenate([-imag_part, real_part], axis=0).astype(jnp.bfloat16)
            right = jnp.concatenate([left, turned], axis=1)
            cross = lax.dot_general(
                left, right, (((0,), (0,)), ((), ())), preferred_element_type=jnp.float32
            )
            cross_real = cross[:, :total]
            cross_imag = cross[:, total:]
            power = jnp.where(diagonal, cross_real, 0.0)
            root_row = lax.rsqrt(jnp.sum(power, axis=0, keepdims=True) / looks_count + EPS)
            root_col = lax.rsqrt(jnp.sum(power, axis=1, keepdims=True) / looks_count + EPS)
            factor = root_col * root_row * (1.0 / looks_count)
            real = (cross_real * factor).astype(jnp.bfloat16)
            imag = (cross_imag * factor).astype(jnp.bfloat16)
            coherence_ref[0, window] = real
            coherence_ref[1, window] = imag
            z0 = lax.dot_general(
                real, ones, (((1,), (0,)), ((), ())), preferred_element_type=jnp.float32
            )
            z1 = lax.dot_general(
                imag, ones, (((1,), (0,)), ((), ())), preferred_element_type=jnp.float32
            )
            real = real.astype(jnp.float32)
            imag = imag.astype(jnp.float32)
            for iteration in range(1, ITERS + 1):
                axis = iteration % 2 == 0
                power = jnp.sum(z0 * z0 + z1 * z1, axis=int(axis), keepdims=True)
                scale = lax.rsqrt(power / total + EPS)
                if iteration == ITERS:
                    break
                if axis:
                    v0 = z0 * scale
                    v1 = z1 * scale
                    z0 = jnp.sum(real * v0 - imag * v1, axis=1, keepdims=True)
                    z1 = jnp.sum(real * v1 + imag * v0, axis=1, keepdims=True)
                else:
                    z0, z1 = (
                        jnp.sum(real * z0 + imag * z1, axis=0, keepdims=True) * scale,
                        jnp.sum(real * z1 - imag * z0, axis=0, keepdims=True) * scale,
                    )
            vectors[pl.ds(window, 1), :] = z0 * scale
            vectors[pl.ds(per_device + window, 1), :] = z1 * scale

        @pl.when(step == pl.num_programs(0) - 1)
        def _():
            turned = vectors[...].T
            for block in range(blocks):
                kept = turned[block * dates : block * dates + SUB]
                for tile in range(1, date_tiles):
                    start = block * dates + tile * SUB
                    kept = kept + pltpu.roll(
                        turned[start : start + SUB], tile * 2 * per_device, 1
                    )
                packed_ref[block] = kept

    whole = pl.BlockSpec(memory_space=pltpu.VMEM)
    return pl.pallas_call(
        kernel,
        grid=(per_device // per_step,),
        in_specs=[pl.BlockSpec(memory_space=pltpu.SMEM)] + [whole] * blocks,
        out_specs=[
            pl.BlockSpec(memory_space=pltpu.VMEM),
            pl.BlockSpec(memory_space=pltpu.VMEM),
        ],
        out_shape=[
            pltpu.VMEM((2, per_device, total, total), jnp.bfloat16),
            pltpu.VMEM((blocks, SUB, width), jnp.float32),
        ],
        scratch_shapes=[
            pltpu.VMEM((groups, total, width), jnp.bfloat16),
            pltpu.VMEM((per_device, 2, pairs * blocks, total), jnp.float32),
            pltpu.VMEM((width, total), jnp.float32),
        ],
        name="link_windows",
    )(position.astype(jnp.int32).reshape(1), *[on_chip(piece) for piece in pieces])


def unpack_linked(packed, dates, per_device):
    blocks, _, width = packed.shape
    date_tiles = dates // SUB

    def kernel(packed_ref, out_ref):
        lane = lax.broadcasted_iota(jnp.int32, (SUB, width), 1)
        owner = lax.div(lane, per_device)
        for part in range(2):
            for tile in range(date_tiles):
                held = (tile * 2 + part) * per_device
                row = jnp.zeros((SUB, width), jnp.float32)
                for source in range(blocks):
                    shift = (source * per_device - held) % width
                    moved = packed_ref[source]
                    if shift:
                        moved = pltpu.roll(moved, shift, 1)
                    row = jnp.where(owner == source, moved, row)
                out_ref[part, tile * SUB : (tile + 1) * SUB, :] = row

    return pl.pallas_call(
        kernel,
        in_specs=[pl.BlockSpec(memory_space=pltpu.VMEM)],
        out_specs=pl.BlockSpec(memory_space=pltpu.VMEM),
        out_shape=jax.ShapeDtypeStruct((2, dates, width), jnp.float32),
        name="unpack_linked",
    )(on_chip(packed))


def local(slc, usable):
    looks_count = slc.shape[1]
    own_dates = slc.shape[2]
    windows = slc.shape[3]
    blocks = lax.axis_size("date")
    per_device = windows // blocks
    position = lax.axis_index("date")
    chunk = blocks // 2
    extra = -looks_count % chunk
    if extra:
        slc = jnp.pad(slc, ((0, 0), (0, extra), (0, 0), (0, 0)))
        usable = jnp.pad(usable, ((0, extra), (0, 0), (0, 0)))
    order = sorted(range(1, blocks), key=lambda hop: abs(hop - blocks // 2)) + [0]
    pieces = pack_blocks(slc, usable, position, order)
    received = []
    for hop, piece in zip(order, pieces):
        pairs = [(source, (source + hop) % blocks) for source in range(blocks)]
        received.append(lax.ppermute(piece, "date", pairs) if hop else piece)
    coherence, packed = link_windows(received, order, position, looks_count, per_device)
    packed = lax.all_to_all(packed, "date", split_axis=0, concat_axis=0, tiled=True)
    linked = unpack_linked(packed, own_dates, per_device)
    total = own_dates * blocks
    return (coherence.reshape(2, 1, 1, per_device, total, total), linked)


def solution(mesh):
    return jax.shard_map(
        local,
        mesh=mesh,
        in_specs=(
            P(None, None, "date", ("slab", "tile", "sub")),
            P(None, "date", ("slab", "tile", "sub")),
        ),
        out_specs=(
            P(None, ("slab", "tile", "sub"), "date", None, None, None),
            P(None, "date", ("slab", "tile", "sub")),
        ),
        check_vma=False,
    )
```

```python
import jax
import jax.numpy as jnp
from jax import lax
from jax.experimental import pallas as pl
from jax.experimental.pallas import tpu as pltpu
from jax.sharding import PartitionSpec as P

ITERS = 4
EPS = 1e-05
SUB = 8


def on_chip(array):
    return pltpu.with_memory_space_constraint(array, pltpu.VMEM)


def pack_blocks(slc, usable, position, order):
    blocks = len(order)
    parts, looks, dates, windows = slc.shape
    per_device = windows // blocks
    chunk = blocks // parts
    groups = looks // chunk
    per_step = max(n for n in range(1, 6) if groups % n == 0)

    steps = groups // per_step
    span = per_step * chunk

    def kernel(shift_ref, slc_source, usable_source, *refs):
        out_refs = refs[:blocks]
        slc_ref, usable_ref, sems = refs[blocks:]
        shift = shift_ref[0]
        lane = lax.broadcasted_iota(jnp.int32, (dates, windows), 1).astype(jnp.int16)

        def loads(step):
            at = pl.ds(step * span, span)
            return [
                pltpu.make_async_copy(slc_source.at[part, at], slc_ref.at[part, at], sems.at[part, step])
                for part in range(parts)
            ] + [pltpu.make_async_copy(usable_source.at[at], usable_ref.at[at], sems.at[parts, step])]

        for step in range(steps):
            for load in loads(step):
                load.start()
        for step in range(steps):
            for load in loads(step):
                load.wait()
            for group in range(step * per_step, (step + 1) * per_step):
                rows = []
                flags = [usable_ref[group * chunk + look].astype(jnp.bfloat16) for look in range(chunk)]
                for part in range(parts):
                    for look in range(chunk):
                        sample = slc_ref[part, group * chunk + look]
                        rows.append(pltpu.roll(sample * flags[look], shift, 1))
                stride = blocks // 2
                while stride:
                    width = stride * per_device
                    low_half = (lane & width) == 0
                    for index in range(blocks):
                        if index & stride:
                            continue
                        low, high = rows[index], rows[index + stride]
                        rows[index] = jnp.where(low_half, low, pltpu.roll(high, width, 1))
                        rows[index + stride] = jnp.where(
                            low_half, pltpu.roll(low, windows - width, 1), high
                        )
                    stride //= 2
                for index, hop in enumerate(order):
                    out_refs[index][group] = rows[hop]

    piece = pltpu.VMEM((groups, dates, windows), jnp.bfloat16)
    shift = (windows - per_device * position) % windows
    return pl.pallas_call(
        kernel,
        in_specs=[
            pl.BlockSpec(memory_space=pltpu.SMEM),
            pl.BlockSpec(memory_space=pl.ANY),
            pl.BlockSpec(memory_space=pl.ANY),
        ],
        out_specs=[pl.BlockSpec(memory_space=pltpu.VMEM)] * blocks,
        out_shape=[piece] * blocks,
        scratch_shapes=[
            pltpu.VMEM(slc.shape, slc.dtype),
            pltpu.VMEM(usable.shape, usable.dtype),
            pltpu.SemaphoreType.DMA((parts + 1, steps)),
        ],
        name="pack_blocks",
    )(shift.astype(jnp.int32).reshape(1), slc, usable)


def link_windows(pieces, order, position, looks_count, per_device):
    blocks = len(pieces)
    groups, dates, width = pieces[0].shape
    total = blocks * dates
    pairs = (groups + 1) // 2
    half = blocks // 2
    date_tiles = dates // SUB
    per_step = 4

    def kernel(position_ref, *refs):
        piece_refs = refs[:blocks]
        coherence_ref, packed_ref, stacked, samples, vectors = refs[blocks:]
        step = pl.program_id(0)

        @pl.when(step == 0)
        def _():
            for index, hop in enumerate(order):
                source = lax.rem(position_ref[0] + (blocks - hop), blocks)
                start = pl.multiple_of(source * dates, dates)
                stacked[:, pl.ds(start, dates), :] = piece_refs[index][...]
            row = lax.broadcasted_iota(jnp.int32, (2 * width, 2 * width), 0)
            col = lax.broadcasted_iota(jnp.int32, (2 * width, 2 * width), 1)
            inner = lax.rem(col, width)
            slot = lax.div(inner, per_device)
            wanted = (
                lax.rem(inner, per_device) * (2 * blocks)
                + lax.div(slot, half) * blocks
                + lax.div(col, width) * half
                + lax.rem(slot, half)
            )
            select = jnp.where(wanted == row, 1.0, 0.0).astype(jnp.bfloat16)
            for pair in range(pairs):
                first = 2 * pair
                if first + 1 < groups:
                    block = jnp.concatenate([stacked[first], stacked[first + 1]], axis=1)
                    chosen = select
                else:
                    block = stacked[first]
                    chosen = select[:, :width]
                turned = lax.dot_general(
                    chosen, block, (((1,), (1,)), ((), ())), preferred_element_type=jnp.float32
                )
                samples[:, :, pair * blocks : (pair + 1) * blocks, :] = turned.reshape(
                    per_device, 2, blocks, total
                )
            vectors[...] = jnp.zeros_like(vectors)

        ones = jnp.ones((total, total), jnp.bfloat16)
        diagonal = lax.broadcasted_iota(jnp.int32, (total, total), 0) == lax.broadcasted_iota(
            jnp.int32, (total, total), 1
        )
        for index in range(per_step):
            window = step * per_step + index
            real_part = samples[window, 0]
            imag_part = samples[window, 1]
            left = jnp.concatenate([real_part, imag_part], axis=0).astype(jnp.bfloat16)
            turned = jnp.concatenate([-imag_part, real_part], axis=0).astype(jnp.bfloat16)
            right = jnp.concatenate([left, turned], axis=1)
            cross = lax.dot_general(
                left, right, (((0,), (0,)), ((), ())), preferred_element_type=jnp.float32
            )
            cross_real = cross[:, :total]
            cross_imag = cross[:, total:]
            power = jnp.where(diagonal, cross_real, 0.0)
            root_row = lax.rsqrt(jnp.sum(power, axis=0, keepdims=True) / looks_count + EPS)
            root_col = lax.rsqrt(jnp.sum(power, axis=1, keepdims=True) / looks_count + EPS)
            factor = root_col * root_row * (1.0 / looks_count)
            real = (cross_real * factor).astype(jnp.bfloat16)
            imag = (cross_imag * factor).astype(jnp.bfloat16)
            coherence_ref[0, window] = real
            coherence_ref[1, window] = imag
            z0 = lax.dot_general(
                real, ones, (((1,), (0,)), ((), ())), preferred_element_type=jnp.float32
            )
            z1 = lax.dot_general(
                imag, ones, (((1,), (0,)), ((), ())), preferred_element_type=jnp.float32
            )
            real = real.astype(jnp.float32)
            imag = imag.astype(jnp.float32)
            for iteration in range(1, ITERS + 1):
                axis = iteration % 2 == 0
                power = jnp.sum(z0 * z0 + z1 * z1, axis=int(axis), keepdims=True)
                scale = lax.rsqrt(power / total + EPS)
                if iteration == ITERS:
                    break
                if axis:
                    v0 = z0 * scale
                    v1 = z1 * scale
                    z0 = jnp.sum(real * v0 - imag * v1, axis=1, keepdims=True)
                    z1 = jnp.sum(real * v1 + imag * v0, axis=1, keepdims=True)
                else:
                    z0, z1 = (
                        jnp.sum(real * z0 + imag * z1, axis=0, keepdims=True) * scale,
                        jnp.sum(real * z1 - imag * z0, axis=0, keepdims=True) * scale,
                    )
            vectors[pl.ds(window, 1), :] = z0 * scale
            vectors[pl.ds(per_device + window, 1), :] = z1 * scale

        @pl.when(step == pl.num_programs(0) - 1)
        def _():
            turned = vectors[...].T
            for block in range(blocks):
                kept = turned[block * dates : block * dates + SUB]
                for tile in range(1, date_tiles):
                    start = block * dates + tile * SUB
                    kept = kept + pltpu.roll(
                        turned[start : start + SUB], tile * 2 * per_device, 1
                    )
                packed_ref[block] = kept

    whole = pl.BlockSpec(memory_space=pltpu.VMEM)
    return pl.pallas_call(
        kernel,
        grid=(per_device // per_step,),
        in_specs=[pl.BlockSpec(memory_space=pltpu.SMEM)] + [whole] * blocks,
        out_specs=[
            pl.BlockSpec(memory_space=pltpu.VMEM),
            pl.BlockSpec(memory_space=pltpu.VMEM),
        ],
        out_shape=[
            pltpu.VMEM((2, per_device, total, total), jnp.bfloat16),
            pltpu.VMEM((blocks, SUB, width), jnp.float32),
        ],
        scratch_shapes=[
            pltpu.VMEM((groups, total, width), jnp.bfloat16),
            pltpu.VMEM((per_device, 2, pairs * blocks, total), jnp.float32),
            pltpu.VMEM((width, total), jnp.float32),
        ],
        name="link_windows",
    )(position.astype(jnp.int32).reshape(1), *[on_chip(piece) for piece in pieces])


def unpack_linked(packed, dates, per_device):
    blocks, _, width = packed.shape
    date_tiles = dates // SUB

    def kernel(packed_ref, out_ref):
        lane = lax.broadcasted_iota(jnp.int32, (SUB, width), 1)
        owner = lax.div(lane, per_device)
        for part in range(2):
            for tile in range(date_tiles):
                held = (tile * 2 + part) * per_device
                row = jnp.zeros((SUB, width), jnp.float32)
                for source in range(blocks):
                    shift = (source * per_device - held) % width
                    moved = packed_ref[source]
                    if shift:
                        moved = pltpu.roll(moved, shift, 1)
                    row = jnp.where(owner == source, moved, row)
                out_ref[part, tile * SUB : (tile + 1) * SUB, :] = row

    return pl.pallas_call(
        kernel,
        in_specs=[pl.BlockSpec(memory_space=pltpu.VMEM)],
        out_specs=pl.BlockSpec(memory_space=pltpu.VMEM),
        out_shape=jax.ShapeDtypeStruct((2, dates, width), jnp.float32),
        name="unpack_linked",
    )(on_chip(packed))


def local(slc, usable):
    looks_count = slc.shape[1]
    own_dates = slc.shape[2]
    windows = slc.shape[3]
    blocks = lax.axis_size("date")
    per_device = windows // blocks
    position = lax.axis_index("date")
    chunk = blocks // 2
    extra = -looks_count % chunk
    if extra:
        slc = jnp.pad(slc, ((0, 0), (0, extra), (0, 0), (0, 0)))
        usable = jnp.pad(usable, ((0, extra), (0, 0), (0, 0)))
    order = sorted(range(1, blocks), key=lambda hop: abs(hop - blocks // 2)) + [0]
    pieces = pack_blocks(slc, usable, position, order)
    received = []
    for hop, piece in zip(order, pieces):
        pairs = [(source, (source + hop) % blocks) for source in range(blocks)]
        received.append(lax.ppermute(piece, "date", pairs) if hop else piece)
    coherence, packed = link_windows(received, order, position, looks_count, per_device)
    packed = lax.all_to_all(packed, "date", split_axis=0, concat_axis=0, tiled=True)
    linked = unpack_linked(packed, own_dates, per_device)
    total = own_dates * blocks
    return (coherence.reshape(2, 1, 1, per_device, total, total), linked)


def solution(mesh):
    return jax.shard_map(
        local,
        mesh=mesh,
        in_specs=(
            P(None, None, "date", ("slab", "tile", "sub")),
            P(None, "date", ("slab", "tile", "sub")),
        ),
        out_specs=(
            P(None, ("slab", "tile", "sub"), "date", None, None, None),
            P(None, "date", ("slab", "tile", "sub")),
        ),
        check_vma=False,
    )
```
